32 devices in a mesh: expert: 16 (over z, y, core), dp: 2 (over x).
Axes of the slice: x: 2, y: 2, z: 4, core: 2. Of those that a mesh axis runs over, the one named last changes fastest.
Arguments:
- tokens: bfloat16 [4096, 7168], P(('expert', 'dp')), may hold values from -6 to 6
- cotangent: bfloat16 [4096, 7168], P(('expert', 'dp')), may hold values from -1.5 to 1.5
- routes: int32 [4096, 8], P(('expert', 'dp')), may hold values from 0 to 255, all different within a row; in each aligned block of 128 rows (0 to 127, 128 to 255, ...) at most 9 rows name the same one
- route_gates: float32 [4096, 8], P(('expert', 'dp')), may hold values from 0.1 to 1
- gate_weight: bfloat16 [16, 7168, 256], P('expert'), may hold values from -0.0625 to 0.0625
- up_weight: bfloat16 [16, 7168, 256], P('expert'), may hold values from -0.0625 to 0.0625
- down_weight: bfloat16 [16, 256, 7168], P('expert'), may hold values from -0.125 to 0.125
Outputs:
- grad_gate: bfloat16 [16, 7168, 256], P('expert')
- grad_up: bfloat16 [16, 7168, 256], P('expert')
- grad_down: bfloat16 [16, 256, 7168], P('expert')
The draws below stay inside these ranges and needn't reach their ends.
Inputs may be any that keep to these rules, and one draw needn't show every extreme that they name: `routes`: each row names 8 different experts; among the rows of one device no expert is named more than 9 times.
All inputs are finite; a program needn't handle non-finite values.
Results may differ from the reference program's by a relative error of at most 0.0065.
Values may be sent and summed in bfloat16 or wider, within the bound.
No kernel may reach another device: no remote copies, remote signals or barrier semaphores. Data moves between devices by JAX's collectives and lax.ppermute only.
A program may use at most 192 MiB of HBM per device.

```python
import math
import jax
import jax.numpy as jnp
import numpy as np
from jax import lax

D = 7168
EXPERTS = 256
TOP = 8
HIDDEN_SIZE = 2048
SLICE_UNITS = 256
TOK_DEV = 128
CAP = 9
TOKENS = 4096
N_EXPERT = 16
N_DP = 2


def block_scale(stream_key, shape, split, smallest, high):
    level = 1.0
    for dim, shards_of in split:
        draws = jax.random.uniform(jax.random.fold_in(jax.random.fold_in(stream_key, 6), dim), (shards_of,), jnp.float32, smallest / len(split), high / len(split))
        level = level * jnp.repeat(jnp.exp(draws), shape[dim] // shards_of).reshape((-1,) + (1,) * (len(shape) - 1 - dim))
    return level


def assign_block(own_key, own, number, rows, number_of, top, most, lean):
    order = jax.random.permutation(own_key, number_of)
    crowded, common = portions_of(number_of, rows * top, most, lean, True), portions_of(number_of, rows * top, most, lean, False)
    places = jnp.arange(number_of)

    def named(sizes, offset_by):
        used = int((sizes > 0).sum())
        fixed = max(1, used // 4)
        passed = fixed + (places - fixed + offset_by * (used - fixed)) % max(1, number_of - fixed)
        return jnp.zeros((number_of,), jnp.int32).at[order[jnp.where(places < fixed, places, passed)]].set(jnp.asarray(sizes, jnp.int32))

    sizes = jnp.where(number % 4 == 0, named(crowded, number // 4), named(common, number - number // 4 - 1))
    mixed = jax.random.permutation(jax.random.fold_in(own, 3), number_of)
    giver, receiver = mixed[0:number_of // 2 * 2:2], mixed[1:number_of // 2 * 2:2]
    slack = jnp.minimum(sizes[giver] - 1, most - sizes[receiver]) // 2
    slack = jnp.where((giver == order[0]) | (receiver == order[0]) | (sizes[receiver] == 0), 0, jnp.maximum(slack, 0))
    passed = jax.random.randint(jax.random.fold_in(own, 4), (number_of // 2,), 0, 1 << 20) % (slack + 1)
    sizes = sizes.at[giver].add(-passed).at[receiver].add(passed)
    labels = jnp.searchsorted(jnp.cumsum(sizes), jnp.arange(rows * top), side="right").astype(jnp.int32)
    table = labels.reshape(top, rows).T
    table = table[jax.random.permutation(jax.random.fold_in(own, 1), rows)]
    offset_by = jax.random.randint(jax.random.fold_in(own, 2), (rows, 1), 0, top)
    return jnp.take_along_axis(table, (jnp.arange(top)[None, :] + offset_by) % top, axis=1)


def portions_of(amount, total, reach, skew, full):
    loads = [(1 << 20) // math.isqrt(standing ** skew) + 1 for standing in range(1, amount + 1)]
    largest = reach if full else min(reach, max(-(-total // amount), total * loads[0] // sum(loads)))
    least = 1 if total - largest >= amount - 1 else 0
    given, rest = [largest] + [least] * (amount - 1), total - largest - least * (amount - 1)
    while rest > 0:
        candidates = [i for i in range(1, amount) if given[i] < largest] or [i for i in range(1, amount) if given[i] < reach]
        mass, remaining = sum([loads[i] for i in candidates]), rest
        for i in candidates:
            more = min(reach - given[i], max(1, remaining * loads[i] // mass), rest)
            given[i] = given[i] + more
            rest = rest - more
    return np.array(given)


def centred(key, extent, deviation, limit, pieces=(), held_as=jnp.bfloat16):
    result = jax.random.normal(key, extent, jnp.float32) * deviation
    if len(pieces) > 0:
        result = block_scale(key, extent, pieces, -0.22, 0.18) * result
    return jnp.clip(result, min=-limit, max=limit).astype(held_as)


def setup_inputs(seed: int = 0) -> dict:
    key_list = jax.random.split(jax.random.key(seed), 8)
    tokens = centred(key_list[0], (TOKENS, D), 1.0, 6.0, ((0, 32),))
    cotangent = centred(key_list[1], (TOKENS, D), 0.25, 1.5, ((0, 32),))
    routes_keys = jax.random.split(jax.random.fold_in(key_list[2], 1), TOKENS // TOK_DEV)
    routes_turns = jax.random.permutation(jax.random.fold_in(key_list[2], 3), TOKENS // TOK_DEV)
    routes = jax.vmap(lambda own, number: assign_block(jax.random.fold_in(key_list[2], 2), own, number, TOK_DEV, EXPERTS, TOP, CAP, 2))(routes_keys, routes_turns).reshape((TOKENS, TOP))
    route_gates = jnp.clip(0.1 + 0.9 * jax.random.uniform(key_list[3], (TOKENS, TOP), jnp.float32) ** block_scale(key_list[3], (TOKENS, TOP), ((0, 32),), -0.2, 0.2), 0.1, 1.0)
    gate_weight = centred(key_list[4], (N_EXPERT, D, SLICE_UNITS), D ** -0.5, 0.0625, ((0, 16),))
    up_weight = centred(key_list[5], (N_EXPERT, D, SLICE_UNITS), D ** -0.5, 0.0625, ((0, 16),))
    down_weight = centred(key_list[6], (N_EXPERT, SLICE_UNITS, D), HIDDEN_SIZE ** -0.5, 0.125, ((0, 16),))
    return dict(tokens=tokens, cotangent=cotangent, routes=routes, route_gates=route_gates, gate_weight=gate_weight, up_weight=up_weight, down_weight=down_weight)


def expert_grads(inputs, scaled, gate_full, up_full, down_full):
    gate_pre = jnp.dot(inputs, gate_full, preferred_element_type=jnp.float32)
    up_pre = jnp.dot(inputs, up_full, preferred_element_type=jnp.float32)
    sigmoid = jax.nn.sigmoid(gate_pre)
    active = gate_pre * sigmoid
    hidden = (active * up_pre).astype(jnp.bfloat16)
    back_hidden = jnp.dot(scaled, down_full.T, preferred_element_type=jnp.float32)
    gate_delta = (back_hidden * up_pre * sigmoid * (1.0 + gate_pre * (1.0 - sigmoid))).astype(jnp.bfloat16)
    up_delta = (back_hidden * active).astype(jnp.bfloat16)
    gate_term = jnp.dot(inputs.T, gate_delta, preferred_element_type=jnp.float32)
    up_term = jnp.dot(inputs.T, up_delta, preferred_element_type=jnp.float32)
    down_term = jnp.dot(hidden.T, scaled, preferred_element_type=jnp.float32)
    return gate_term, up_term, down_term


def rounded(values):
    return lax.optimization_barrier(values.astype(jnp.bfloat16)).astype(jnp.float32)


def reference(tokens, cotangent, routes, route_gates, gate_weight, up_weight, down_weight):
    slices = HIDDEN_SIZE // SLICE_UNITS
    window = N_EXPERT // slices
    slot_total = N_EXPERT * CAP
    shaped_tokens = tokens.reshape(N_EXPERT, N_DP, TOK_DEV, D)
    shaped_cot = cotangent.reshape(N_EXPERT, N_DP, TOK_DEV, D)
    shaped_routes = routes.reshape(N_EXPERT, N_DP, TOK_DEV, TOP)
    shaped_gates = route_gates.reshape(N_EXPERT, N_DP, TOK_DEV, TOP)
    gate_total, up_total, down_total = None, None, None
    for replica in range(N_DP):
        group_inputs = shaped_tokens[:, replica].reshape(-1, D)
        group_cot = shaped_cot[:, replica].reshape(-1, D)
        group_routes = shaped_routes[:, replica].reshape(-1, TOP)
        group_gates = shaped_gates[:, replica].reshape(-1, TOP)
        gate_list, up_list, down_list = [], [], []
        for expert in range(window):
            matched = group_routes == expert
            chosen = jnp.any(matched, axis=1)
            coefficient = jnp.sum(jnp.where(matched, group_gates, jnp.zeros_like(group_gates)), axis=1)
            picked = jnp.nonzero(chosen, size=slot_total, fill_value=0)[0].astype(jnp.int32)
            live_slot = jnp.arange(slot_total) < jnp.sum(chosen.astype(jnp.int32))
            picked_coef = coefficient[picked]
            weight = jnp.where(live_slot, picked_coef, jnp.zeros_like(picked_coef))
            inputs = group_inputs[picked]
            scaled = (weight[:, None] * group_cot[picked].astype(jnp.float32)).astype(jnp.bfloat16)
            first_slice = expert * slices
            gate_full = jnp.transpose(gate_weight[first_slice:first_slice + slices], (1, 0, 2)).reshape(D, HIDDEN_SIZE)
            up_full = jnp.transpose(up_weight[first_slice:first_slice + slices], (1, 0, 2)).reshape(D, HIDDEN_SIZE)
            down_full = down_weight[first_slice:first_slice + slices].reshape(HIDDEN_SIZE, D)
            gate_term, up_term, down_term = expert_grads(inputs, scaled, gate_full, up_full, down_full)
            gate_list.append(jnp.transpose(gate_term.reshape(D, slices, SLICE_UNITS), (1, 0, 2)))
            up_list.append(jnp.transpose(up_term.reshape(D, slices, SLICE_UNITS), (1, 0, 2)))
            down_list.append(down_term.reshape(slices, SLICE_UNITS, D))
        gate_part = rounded(jnp.concatenate(gate_list, axis=0))
        up_part = rounded(jnp.concatenate(up_list, axis=0))
        down_part = rounded(jnp.concatenate(down_list, axis=0))
        if gate_total is None:
            gate_total, up_total, down_total = gate_part, up_part, down_part
        else:
            gate_total = gate_total + gate_part
            up_total = up_total + up_part
            down_total = down_total + down_part
    return gate_total.astype(jnp.bfloat16), up_total.astype(jnp.bfloat16), down_total.astype(jnp.bfloat16)
```

```python
import jax
import jax.numpy as jnp
from jax import lax
from jax.sharding import PartitionSpec as P

HIDDEN_SIZE = 2048
CAP = 9
LANES = 128
SUBLANES = 8
AXES = ("expert", "dp")


def hop(block, expert_mask, dp_mask):
    experts = lax.axis_size("expert")
    replicas = lax.axis_size("dp")
    route = []
    for e in range(experts):
        for r in range(replicas):
            route.append((e * replicas + r, (e ^ expert_mask) * replicas + (r ^ dp_mask)))
    return lax.ppermute(block, AXES, route)


def bits_of(count):
    return [1 << b for b in range(count.bit_length() - 1)]


def cut(width, parts):
    tiles = width // LANES
    edges = [(tiles * i + parts - 1) // parts * LANES for i in range(parts + 1)]
    return list(zip(edges[:-1], edges[1:]))


def gather_cube(block, dims):
    parts = []
    for p, (low, high) in enumerate(cut(block.shape[-1], len(dims))):
        order = dims[p:] + dims[:p]
        parts.append([block[None, :, low:high], [0], order])
    for level in range(len(dims)):
        for part in parts:
            dim = part[2][level]
            other = hop(part[0], *dim)
            bit = 1 << dims.index(dim)
            part[0] = jnp.concatenate((part[0], other), axis=0)
            part[1] = part[1] + [m ^ bit for m in part[1]]
    return [(stack, masks) for stack, masks, _ in parts]


def in_order(parts):
    sorted_parts = []
    for stack, masks in parts:
        where = [masks.index(m) for m in range(len(masks))]
        sorted_parts.append(jnp.concatenate([stack[w : w + 1] for w in where], axis=0))
    return jnp.concatenate(sorted_parts, axis=2)


def on_device(tokens, cotangent, routes, route_gates, gate_weight, up_weight, down_weight):
    units = gate_weight.shape[2]
    slices = HIDDEN_SIZE // units
    experts_all = lax.axis_size("expert")
    window = experts_all // slices
    width = tokens.shape[1]
    half = width // 2
    top_count = routes.shape[1]
    me = lax.axis_index("expert")
    group = me // slices
    core = me % 2

    flat_routes = routes.reshape(-1)
    flat_gates = route_gates.reshape(-1)
    inside = flat_routes < window
    member = ((flat_routes[:, None] == jnp.arange(window)[None, :]) & inside[:, None]).astype(jnp.int32)
    earlier = jnp.cumsum(member, axis=0) - member
    slot_index = jnp.sum(earlier * member, axis=1)
    relative = jnp.bitwise_xor(flat_routes, group)
    target = jnp.where(inside, relative * CAP + slot_index, -1)
    landing = target[:, None] == jnp.arange(window * CAP)[None, :]
    owning = jnp.arange(flat_routes.shape[0]) // top_count
    source = jnp.sum(jnp.where(landing, owning[:, None], 0), axis=0)
    weight = jnp.sum(jnp.where(landing, flat_gates[:, None], 0.0), axis=0)
    rows = tokens[source]
    scaled = (weight[:, None] * cotangent[source].astype(jnp.float32)).astype(jnp.bfloat16)
    both = jnp.stack((rows, scaled), axis=1).reshape(window, CAP, 2, 2, half)
    mine = lax.dynamic_index_in_dim(both, core, 3, keepdims=False)
    theirs = lax.dynamic_index_in_dim(both, 1 - core, 3, keepdims=False)

    def by_core(own, other):
        return jnp.where(core == 0, jnp.concatenate((own, other), axis=0), jnp.concatenate((other, own), axis=0))

    own = by_core(mine[0], hop(theirs[0], 1, 0)).reshape(2, CAP, 2, half)
    crossed = []
    for delta in range(1, window):
        crossed.append(by_core(hop(mine[delta], delta * slices, 0), hop(theirs[delta], delta * slices + 1, 0)))
    main = CAP // SUBLANES * SUBLANES
    first = own[:, :main].reshape(2 * main, 2, half)
    second = jnp.concatenate(crossed + [own[:, main:].reshape(-1, 2, half)], axis=0)

    dims = [(0, m) for m in bits_of(lax.axis_size("dp"))] + [(m, 0) for m in bits_of(slices)[1:]]
    pieces = []
    for slab in (first, second):
        count = slab.shape[0]
        count += -count % (SUBLANES // 2)
        slab = jnp.pad(slab, ((0, count - slab.shape[0]), (0, 0), (0, 0)))
        block = jnp.transpose(slab, (1, 0, 2)).reshape(2 * count, half)
        parts = gather_cube(block, dims)
        others = [(hop(stack, 1, 0), masks) for stack, masks in parts]
        mine_all = in_order(parts)
        other_all = in_order(others)
        full = jnp.where(
            core == 0,
            jnp.concatenate((mine_all, other_all), axis=2),
            jnp.concatenate((other_all, mine_all), axis=2),
        )
        up_to = -(-count // SUBLANES) * SUBLANES
        start = count // SUBLANES * SUBLANES
        pieces.append((full[:, :up_to].reshape(-1, width), full[:, start:].reshape(-1, width), count, up_to, start))

    gate_full, up_full, down_full = gate_weight[0], up_weight[0], down_weight[0]
    lefts, rights, deltas, hiddens = [], [], [], []
    for inputs, scaled_rows, count, up_to, start in pieces:
        shift = count - start
        gate_pre = jnp.dot(inputs, gate_full, preferred_element_type=jnp.float32)
        up_pre = jnp.dot(inputs, up_full, preferred_element_type=jnp.float32)
        back = lax.dot_general(scaled_rows, down_full, (((1,), (1,)), ((), ())), preferred_element_type=jnp.float32)
        if shift:
            back = jnp.roll(back, -shift, axis=0)
        live = (jnp.arange(inputs.shape[0]) % up_to < count)[:, None]
        sigmoid = jax.nn.sigmoid(gate_pre)
        active = gate_pre * sigmoid
        hidden = jnp.where(live, active * up_pre, 0.0)
        if shift:
            hidden = jnp.roll(hidden, shift, axis=0)
        gate_delta = jnp.where(live, back * up_pre * sigmoid * (1.0 + gate_pre * (1.0 - sigmoid)), 0.0)
        up_delta = jnp.where(live, back * active, 0.0)
        deltas.append(jnp.concatenate((gate_delta, up_delta), axis=1).astype(jnp.bfloat16))
        hiddens.append(hidden.astype(jnp.bfloat16))
        lefts.append(inputs)
        rights.append(scaled_rows)
    inputs = jnp.concatenate(lefts, axis=0)
    scaled_rows = jnp.concatenate(rights, axis=0)
    delta = jnp.concatenate(deltas, axis=0)
    hidden = jnp.concatenate(hiddens, axis=0)
    across = (((0,), (0,)), ((), ()))
    grad_gate = lax.dot_general(inputs, delta[:, :units], across, preferred_element_type=jnp.float32)
    grad_up = lax.dot_general(inputs, delta[:, units:], across, preferred_element_type=jnp.float32)
    grad_down = lax.dot_general(hidden, scaled_rows, across, preferred_element_type=jnp.float32)
    return tuple(g.astype(jnp.bfloat16)[None] for g in (grad_gate, grad_up, grad_down))


def solution(mesh):
    split = P(("expert", "dp"), None)
    held = P("expert", None, None)
    return jax.shard_map(
        on_device,
        mesh=mesh,
        in_specs=(split, split, split, split, held, held, held),
        out_specs=(held, held, held),
        check_vma=False,
    )
```

```python
import functools

import jax
import jax.numpy as jnp
from jax import lax
from jax.experimental import pallas as pl
from jax.experimental.pallas import tpu as pltpu
from jax.sharding import PartitionSpec as P


HIDDEN_SIZE = 2048
CAP = 9
LANES = 128
SUBLANES = 8
AXES = ("expert", "dp")
KERNEL_VMEM = 28 * 1024 * 1024
PIECE = 1280


def hop(block, even, odd=None):
    experts = lax.axis_size("expert")
    replicas = lax.axis_size("dp")
    route = []
    for e in range(experts):
        flip, turn = even if odd is None or e % 2 == 0 else odd
        for r in range(replicas):
            route.append((e * replicas + r, (e ^ flip) * replicas + (r ^ turn)))
    return lax.ppermute(block, AXES, route)


def bits_of(count):
    return [1 << b for b in range(count.bit_length() - 1)]


def cut(width, parts):
    tiles = width // LANES
    edges = [(tiles * i + parts - 1) // parts * LANES for i in range(parts + 1)]
    return list(zip(edges[:-1], edges[1:]))


def turned(dims, by):
    order = dims[::-1]
    order = order[-1:] + order[:-1]
    by = by % len(order)
    return order[by:] + order[:by]


def masks_of(order, dims):
    found = [0]
    for dim in order:
        found = found + [m ^ 1 << dims.index(dim) for m in found]
    return found


def gather_cube(blocks, orders):
    stacks = [b[None] for b in blocks]
    last = len(orders[0][0]) - 1
    for level in range(last + 1):
        others = []
        for stack, order in zip(stacks, orders):
            others.append(hop(stack, order[0][level], order[1][level]))
        if level < last:
            stacks = lax.optimization_barrier([jnp.concatenate(pair, axis=0) for pair in zip(stacks, others)])
    return list(zip(stacks, lax.optimization_barrier(others)))


def dot(a, b, over):
    return lax.dot_general(a, b, (over, ((), ())), preferred_element_type=jnp.float32)


def one_hot(mask):
    return jnp.where(mask, 1.0, 0.0).astype(jnp.bfloat16)


def pick_kernel(window, folds, group_ref, routes_ref, gates_ref, tokens_ref, cotangent_ref, *outs):
    count = tokens_ref.shape[0]
    fold = tokens_ref.shape[1] // folds
    span = 2 * CAP * folds
    routes, gates = routes_ref[...], gates_ref[...]
    ahead = one_hot(
        lax.broadcasted_iota(jnp.int32, (count, count), 0) < lax.broadcasted_iota(jnp.int32, (count, count), 1)
    )
    place = lax.broadcasted_iota(jnp.int32, (span, count), 0)
    row = place % (2 * CAP)
    slot = row % CAP
    inputs_at, scaled_at, weights = [], [], []
    for k in range(window):
        match = routes == (group_ref[0] ^ k)
        chosen = jnp.sum(jnp.where(match, 1.0, 0.0), axis=0, keepdims=True)
        scale = jnp.sum(jnp.where(match, gates, 0.0), axis=0, keepdims=True)
        rank = dot(jnp.broadcast_to(chosen, (SUBLANES, count)).astype(jnp.bfloat16), ahead, ((1,), (0,)))[:1]
        hit = (rank == slot.astype(jnp.float32)) & (chosen > 0.0)
        inputs_at.append(hit & (row < CAP))
        scaled_at.append(hit & (row >= CAP))
        weights.append(jnp.sum(jnp.where(scaled_at[-1], scale, 0.0), axis=1, keepdims=True))
    weight = jnp.concatenate(weights, axis=0)
    total = jnp.zeros((window * span, fold), jnp.float32)
    for f in range(folds):
        here = place // (2 * CAP) == f
        where = pl.ds(f * fold, fold)
        left = jnp.concatenate([one_hot(hit & here) for hit in inputs_at], axis=0)
        right = jnp.concatenate([one_hot(hit & here) for hit in scaled_at], axis=0)
        total += dot(left, tokens_ref[:, where], ((1,), (0,)))
        total += weight * dot(right, cotangent_ref[:, where], ((1,), (0,)))
    for k, out in enumerate(outs):
        out[...] = total[k * span : (k + 1) * span].astype(jnp.bfloat16)


def join_kernel(folds, edges, entries, core_ref, *refs):
    outs = refs[-len(edges) :]
    sources = refs[: -len(edges)]
    core = core_ref[0]
    rows = outs[0].shape[0]
    span = sources[0].shape[0]
    place = lax.broadcasted_iota(jnp.int32, (rows, span), 0)
    item = lax.broadcasted_iota(jnp.int32, (rows, span), 1)
    slot = item % CAP
    quarters = []
    for f in range(folds // 2):
        total = jnp.zeros((rows, sources[0].shape[1]), jnp.float32)
        for source, (flip, low, high, start) in zip(sources, entries):
            base = start + (core ^ flip) * (high - low) - low
            goal = item % (2 * CAP) // CAP * (rows // 2) + base + slot
            taken = (item // (2 * CAP) == core * (folds // 2) + f) & (place == goal) & (slot >= low) & (slot < high)
            total += dot(one_hot(taken), source[...], ((1,), (0,)))
        quarters.append(total.astype(jnp.bfloat16))
    whole = jnp.concatenate(quarters, axis=1)
    for out, (low, high) in zip(outs, edges):
        out[...] = whole[:, low:high]


class Plan:
    def __init__(self, count, places, edges, half):
        self.count = count
        self.rows = -(-count // (2 * SUBLANES)) * 2 * SUBLANES
        self.start = 2 * count - self.rows
        self.shift = count - self.start
        self.places = places
        self.chips = len(places[0][0])
        self.edges = edges
        self.half = half

    def chip(self, side, part, place):
        even, odd = self.places[part][0][place], self.places[part][1][place]
        return even if even == odd else jnp.where(side == 0, even, odd)

    def take(self, pair, low, width, scaled):
        first = self.start if scaled else 0
        found = [ref[:, first : first + self.rows, low : low + width].reshape(-1, width) for ref in pair]
        return jnp.concatenate(found, axis=0)


def in_pairs(flat, parts):
    return [[flat[(lineage * parts + p) * 2 : (lineage * parts + p) * 2 + 2] for p in range(parts)] for lineage in range(2)]


def forward(plan, pairs, core, weights, held, sems, pre):
    gate_held, up_held, down_held = held
    rows, chips, units = plan.rows, plan.chips, gate_held.shape[1]
    steps = []
    for lineage in range(2):
        for p, (low, high) in enumerate(plan.edges):
            side = core ^ lineage
            where = pl.ds(pl.multiple_of(side * plan.half + low, LANES), high - low)
            spots = [(where, slice(None)), (where, slice(None)), (slice(None), where)]
            copies = [
                pltpu.make_async_copy(w.at[at], h.at[at], sems.at[len(steps), i])
                for i, (w, h, at) in enumerate(zip(weights, held, spots))
            ]
            for copy in copies:
                copy.start()
            steps.append((lineage, p, low, high, side, where, copies))
    for lineage, p, low, high, side, where, copies in steps:
        for copy in copies:
            copy.wait()
        inputs = plan.take(pairs[lineage][p], 0, high - low, False)
        scaled = plan.take(pairs[lineage][p], 0, high - low, True)
        sums = (
            dot(inputs, gate_held[where, :], ((1,), (0,))),
            dot(inputs, up_held[where, :], ((1,), (0,))),
            dot(scaled, down_held[:, where], ((1,), (1,))),
        )
        for place in range(chips):
            m = plan.chip(side, p, place)
            for i, value in enumerate(sums):
                part = value[place * rows : (place + 1) * rows]
                pre[i, m] = part if lineage + p == 0 else pre[i, m] + part
    gate_pre, up_pre, back = [pre[i].reshape(chips * rows, units) for i in range(3)]
    total = chips * rows
    if plan.shift:
        back = pltpu.roll(back, total - plan.shift, 0)
    live = lax.broadcasted_iota(jnp.int32, (total, units), 0) % rows < plan.count
    sigmoid = 1.0 / (1.0 + jnp.exp(-gate_pre))
    active = gate_pre * sigmoid
    hidden = jnp.where(live, active * up_pre, 0.0)
    if plan.shift:
        hidden = pltpu.roll(hidden, plan.shift, 0)
    gate_delta = jnp.where(live, back * up_pre * sigmoid * (1.0 + gate_pre * (1.0 - sigmoid)), 0.0)
    up_delta = jnp.where(live, back * active, 0.0)
    return [v.astype(jnp.bfloat16).reshape(chips, rows, units) for v in (gate_delta, up_delta, hidden)]


def first_kernel(plan, core_ref, gate_ref, up_ref, down_ref, *rest):
    parts = len(plan.edges)
    pairs = in_pairs(rest[: 4 * parts], parts)
    delta_ref, hidden_ref, pre, gate_held, up_held, down_held, sems = rest[4 * parts :]
    units = gate_held.shape[1]
    held = (gate_held, up_held, down_held)
    gate_delta, up_delta, hidden = forward(plan, pairs, core_ref[0], (gate_ref, up_ref, down_ref), held, sems, pre)
    delta_ref[:, :, :units] = gate_delta
    delta_ref[:, :, units:] = up_delta
    hidden_ref[...] = hidden


def second_kernel(plans, core_ref, first_delta, first_hidden, gate_ref, up_ref, down_ref, *rest):
    first, second = plans
    parts = len(first.edges)
    first_pairs = in_pairs(rest[: 4 * parts], parts)
    second_pairs = in_pairs(rest[4 * parts : 8 * parts], parts)
    gate_out, up_out, down_out, delta_ref, hidden_ref, pre, gate_held, up_held, down_held, sems, tall, wide, tall_sem, wide_sem = rest[8 * parts :]
    core = core_ref[0]
    chips, units = second.chips, gate_held.shape[1]
    held = (gate_held, up_held, down_held)
    gate_delta, up_delta, hidden = forward(second, second_pairs, core, (gate_ref, up_ref, down_ref), held, sems, pre)
    delta_ref[:, :, :units] = gate_delta
    delta_ref[:, :, units:] = up_delta
    hidden_ref[...] = hidden
    flying = [[], []]
    turn = 0
    for lineage in range(2):
        side = core ^ lineage
        for p, (begin, end) in enumerate(first.edges):
            order = [first.chip(side, p, place) for place in range(chips)]
            delta = jnp.concatenate([first_delta[m] for m in order] + [delta_ref[m] for m in order], axis=0)
            hidden = jnp.concatenate([first_hidden[m] for m in order] + [hidden_ref[m] for m in order], axis=0)
            for low, high in cut(end - begin, -(-(end - begin) // PIECE)):
                width = high - low
                where = pl.ds(pl.multiple_of(side * first.half + begin + low, LANES), width)
                slot = turn % 2
                turn += 1
                for copy in flying[slot]:
                    copy.wait()

                def rows_of(scaled):
                    return jnp.concatenate(
                        (
                            first.take(first_pairs[lineage][p], low, width, scaled),
                            second.take(second_pairs[lineage][p], low, width, scaled),
                        ),
                        axis=0,
                    )

                both = dot(rows_of(False), delta, ((0,), (0,))).astype(jnp.bfloat16)
                tall[slot, 0, :width, :] = both[:, :units]
                tall[slot, 1, :width, :] = both[:, units:]
                wide[slot, :, :width] = dot(hidden, rows_of(True), ((0,), (0,))).astype(jnp.bfloat16)
                copies = [
                    pltpu.make_async_copy(tall.at[slot, 0, pl.ds(0, width), :], gate_out.at[where, :], tall_sem.at[slot, 0]),
                    pltpu.make_async_copy(tall.at[slot, 1, pl.ds(0, width), :], up_out.at[where, :], tall_sem.at[slot, 1]),
                    pltpu.make_async_copy(wide.at[slot, :, pl.ds(0, width)], down_out.at[:, where], wide_sem.at[slot]),
                ]
                for copy in copies:
                    copy.start()
                flying[slot] = copies
    for copies in flying:
        for copy in copies:
            copy.wait()


def on_device(tokens, cotangent, routes, route_gates, gate_weight, up_weight, down_weight):
    units = gate_weight.shape[2]
    slices = HIDDEN_SIZE // units
    window = lax.axis_size("expert") // slices
    width = tokens.shape[1]
    half = width // 2
    me = lax.axis_index("expert").astype(jnp.int32)
    group = (me // slices).reshape(1)
    core = (me % 2).reshape(1)
    smem = pl.BlockSpec(memory_space=pltpu.SMEM)
    vmem = pl.BlockSpec(memory_space=pltpu.VMEM)
    hbm = pl.BlockSpec(memory_space=pl.ANY)

    def near(arrays):
        return [pltpu.with_memory_space_constraint(x, pltpu.VMEM) for x in arrays]

    params = pltpu.CompilerParams(vmem_limit_bytes=KERNEL_VMEM)
    folds = 2
    while 2 * CAP * folds % SUBLANES:
        folds *= 2
    span = 2 * CAP * folds
    picked = pl.pallas_call(
        functools.partial(pick_kernel, window, folds),
        out_shape=(jax.ShapeDtypeStruct((span, width // folds), jnp.bfloat16),) * window,
        in_specs=[smem] + [vmem] * 4,
        out_specs=(vmem,) * window,
        compiler_params=params,
    )(group, routes.T, route_gates.T, tokens, cotangent)
    weights = [pltpu.with_memory_space_constraint(w[0], pltpu.HBM) for w in (gate_weight, up_weight, down_weight)]
    partner = (1, 0)
    landed = [picked[0]]
    for k in range(1, window):
        landed.append(hop(picked[k], (k * slices, 0)))
    pairs = []
    for block in landed:
        pairs.append((block, hop(block, partner)))

    dims = [(0, m) for m in bits_of(lax.axis_size("dp"))] + [(m, 0) for m in bits_of(slices)[1:]]
    tiles = half // LANES
    major = -(-2 * tiles // len(dims)) * LANES
    edges = [(0, major), (major, half)]
    orders = [(turned(dims, 0), turned(dims, 2)), (turned(dims, 1), turned(dims, 1))]
    places = [tuple(masks_of(o, dims) for o in order) for order in orders]
    main = CAP // SUBLANES * SUBLANES
    early = [(0, 0, main, 0)]
    late = [(k, 0, CAP, (k - 1) * 2 * CAP) for k in range(1, window)]
    if main < CAP:
        late.append((0, main, CAP, (window - 1) * 2 * CAP))
    plans, operands, gathered = [], [], []
    for taken in (early, late):
        count = sum(2 * (high - low) for _, low, high, _ in taken)
        count += -count % (SUBLANES // 2)
        sources = [x for k, _, _, _ in taken for x in pairs[k]]
        entries = [(flip, low, high, start) for _, low, high, start in taken for flip in range(2)]
        blocks = pl.pallas_call(
            functools.partial(join_kernel, folds, edges, entries),
            out_shape=tuple(jax.ShapeDtypeStruct((2 * count, high - low), jnp.bfloat16) for low, high in edges),
            in_specs=[smem] + [vmem] * len(sources),
            out_specs=(vmem,) * len(edges),
            compiler_params=params,
        )(core, *near(sources))
        halves = gather_cube(blocks, orders)
        gathered.append(halves)
        stacks = [s for pair in halves for s in pair]
        crossed = []
        for stack in stacks:
            crossed.append(hop(stack, partner))
        operands.append(stacks + crossed)
        plans.append(Plan(count, places, edges, half))

    chips = plans[0].chips

    def delta_shapes(plan, make):
        return [make((chips, plan.rows, 2 * units), jnp.bfloat16), make((chips, plan.rows, units), jnp.bfloat16)]

    def forward_scratch(plan):
        return [
            pltpu.VMEM((3, chips, plan.rows, units), jnp.float32),
            pltpu.VMEM((width, units), jnp.bfloat16),
            pltpu.VMEM((width, units), jnp.bfloat16),
            pltpu.VMEM((units, width), jnp.bfloat16),
            pltpu.SemaphoreType.DMA((2 * len(edges), 3)),
        ]

    flops = [6 * chips * plan.rows * width * units for plan in plans]
    operands[0], _ = lax.optimization_barrier((operands[0], gathered[1][0][0]))
    first = pl.pallas_call(
        functools.partial(first_kernel, plans[0]),
        out_shape=tuple(delta_shapes(plans[0], jax.ShapeDtypeStruct)),
        in_specs=[smem] + [hbm] * 3 + [vmem] * len(operands[0]),
        out_specs=(vmem, vmem),
        scratch_shapes=forward_scratch(plans[0]),
        cost_estimate=pl.CostEstimate(flops=flops[0], bytes_accessed=6 * width * units, transcendentals=0),
        compiler_params=params,
    )(core, *weights, *near(operands[0]))
    grads = pl.pallas_call(
        functools.partial(second_kernel, plans),
        out_shape=(
            jax.ShapeDtypeStruct((width, units), jnp.bfloat16),
            jax.ShapeDtypeStruct((width, units), jnp.bfloat16),
            jax.ShapeDtypeStruct((units, width), jnp.bfloat16),
        ),
        in_specs=[smem] + [vmem] * 2 + [hbm] * 3 + [vmem] * (len(operands[0]) + len(operands[1])),
        out_specs=(hbm, hbm, hbm),
        scratch_shapes=delta_shapes(plans[1], pltpu.VMEM)
        + forward_scratch(plans[1])
        + [
            pltpu.VMEM((2, 2, PIECE, units), jnp.bfloat16),
            pltpu.VMEM((2, units, PIECE), jnp.bfloat16),
            pltpu.SemaphoreType.DMA((2, 2)),
            pltpu.SemaphoreType.DMA((2,)),
        ],
        cost_estimate=pl.CostEstimate(flops=2 * sum(flops), bytes_accessed=12 * width * units, transcendentals=0),
        compiler_params=params,
    )(core, *near(first), *weights, *near(operands[0]), *near(operands[1]))
    return tuple(g[None] for g in grads)


def solution(mesh):
    split = P(("expert", "dp"), None)
    held = P("expert", None, None)

    return jax.shard_map(
        on_device,
        mesh=mesh,
        in_specs=(split, split, split, split, held, held, held),
        out_specs=(held, held, held),
        check_vma=False,
    )
```

```python
import functools

import jax
import jax.numpy as jnp
from jax import lax
from jax.experimental import pallas as pl
from jax.experimental.pallas import tpu as pltpu
from jax.sharding import PartitionSpec as P


HIDDEN_SIZE = 2048
CAP = 9
LANES = 128
SUBLANES = 8
AXES = ("expert", "dp")
KERNEL_VMEM = 18 * 1024 * 1024
PICK_VMEM = 40 * 1024 * 1024
PIECE = 1280


def hop(block, even, odd=None):
    experts = lax.axis_size("expert")
    replicas = lax.axis_size("dp")
    route = []
    for e in range(experts):
        flip, turn = even if odd is None or e % 2 == 0 else odd
        for r in range(replicas):
            route.append((e * replicas + r, (e ^ flip) * replicas + (r ^ turn)))
    return lax.ppermute(block, AXES, route)


def bits_of(count):
    return [1 << b for b in range(count.bit_length() - 1)]


def cut(width, parts):
    tiles = width // LANES
    edges = [(tiles * i + parts - 1) // parts * LANES for i in range(parts + 1)]
    return list(zip(edges[:-1], edges[1:]))


def turned(dims, by):
    order = dims[::-1]
    order = order[-1:] + order[:-1]
    by = by % len(order)
    return order[by:] + order[:by]


def masks_of(order, dims):
    found = [0]
    for dim in order:
        found = found + [m ^ 1 << dims.index(dim) for m in found]
    return found


def gather_cube(blocks, orders):
    stacks = [b[None] for b in blocks]
    last = len(orders[0][0]) - 1
    for level in range(last + 1):
        others = []
        for stack, order in zip(stacks, orders):
            others.append(hop(stack, order[0][level], order[1][level]))
        if level < last:
            stacks = lax.optimization_barrier([jnp.concatenate(pair, axis=0) for pair in zip(stacks, others)])
    return list(zip(stacks, lax.optimization_barrier(others)))


def dot(a, b, over):
    return lax.dot_general(a, b, (over, ((), ())), preferred_element_type=jnp.float32)


def one_hot(mask):
    return jnp.where(mask, 1.0, 0.0).astype(jnp.bfloat16)


def pick_kernel(window, folds, group_ref, routes_hbm, gates_hbm, tokens_hbm, cotangent_hbm, *rest):
    outs = rest[:window]
    routes_ref, gates_ref, tokens_ref, cotangent_ref, small_sem, sems = rest[window:]
    small = [
        pltpu.make_async_copy(routes_hbm, routes_ref, small_sem.at[0]),
        pltpu.make_async_copy(gates_hbm, gates_ref, small_sem.at[1]),
    ]
    copies = []
    for f in range(folds):
        where = pl.ds(f * (tokens_ref.shape[1] // folds), tokens_ref.shape[1] // folds)
        copies.append(
            [
                pltpu.make_async_copy(source.at[:, where], target.at[:, where], sems.at[f, i])
                for i, (source, target) in enumerate(((tokens_hbm, tokens_ref), (cotangent_hbm, cotangent_ref)))
            ]
        )
    for copy in small + [c for pair in copies for c in pair]:
        copy.start()
    for copy in small:
        copy.wait()
    count = tokens_ref.shape[0]
    fold = tokens_ref.shape[1] // folds
    span = 2 * CAP * folds
    routes, gates = routes_ref[...], gates_ref[...]
    ahead = one_hot(
        lax.broadcasted_iota(jnp.int32, (count, count), 0) < lax.broadcasted_iota(jnp.int32, (count, count), 1)
    )
    place = lax.broadcasted_iota(jnp.int32, (span, count), 0)
    row = place % (2 * CAP)
    slot = row % CAP
    inputs_at, scaled_at, weights = [], [], []
    for k in range(window):
        match = routes == (group_ref[0] ^ k)
        chosen = jnp.sum(jnp.where(match, 1.0, 0.0), axis=0, keepdims=True)
        scale = jnp.sum(jnp.where(match, gates, 0.0), axis=0, keepdims=True)
        rank = dot(jnp.broadcast_to(chosen, (SUBLANES, count)).astype(jnp.bfloat16), ahead, ((1,), (0,)))[:1]
        hit = (rank == slot.astype(jnp.float32)) & (chosen > 0.0)
        inputs_at.append(hit & (row < CAP))
        scaled_at.append(hit & (row >= CAP))
        weights.append(jnp.sum(jnp.where(scaled_at[-1], scale, 0.0), axis=1, keepdims=True))
    weight = jnp.concatenate(weights, axis=0)
    total = jnp.zeros((window * span, fold), jnp.float32)
    for f in range(folds):
        here = place // (2 * CAP) == f
        where = pl.ds(f * fold, fold)
        left = jnp.concatenate([one_hot(hit & here) for hit in inputs_at], axis=0)
        right = jnp.concatenate([one_hot(hit & here) for hit in scaled_at], axis=0)
        for copy in copies[f]:
            copy.wait()
        total += dot(left, tokens_ref[:, where], ((1,), (0,)))
        total += weight * dot(right, cotangent_ref[:, where], ((1,), (0,)))
    for k, out in enumerate(outs):
        out[...] = total[k * span : (k + 1) * span].astype(jnp.bfloat16)


def join_kernel(folds, edges, entries, core_ref, *refs):
    outs = refs[-len(edges) :]
    sources = refs[: -len(edges)]
    core = core_ref[0]
    rows = outs[0].shape[0]
    span = sources[0].shape[0]
    place = lax.broadcasted_iota(jnp.int32, (rows, span), 0)
    item = lax.broadcasted_iota(jnp.int32, (rows, span), 1)
    slot = item % CAP
    quarters = []
    for f in range(folds // 2):
        total = jnp.zeros((rows, sources[0].shape[1]), jnp.float32)
        for source, (flip, low, high, start) in zip(sources, entries):
            base = start + (core ^ flip) * (high - low) - low
            goal = item % (2 * CAP) // CAP * (rows // 2) + base + slot
            taken = (item // (2 * CAP) == core * (folds // 2) + f) & (place == goal) & (slot >= low) & (slot < high)
            total += dot(one_hot(taken), source[...], ((1,), (0,)))
        quarters.append(total.astype(jnp.bfloat16))
    whole = jnp.concatenate(quarters, axis=1)
    for out, (low, high) in zip(outs, edges):
        out[...] = whole[:, low:high]


def load_kernel(count, *refs):
    sems = refs[-1]
    copies = [pltpu.make_async_copy(refs[i], refs[count + 1 + i], sems.at[i]) for i in range(count)]
    for copy in copies:
        copy.start()
    for copy in copies:
        copy.wait()


class Plan:
    def __init__(self, count, places, edges, half):
        self.count = count
        self.rows = -(-count // SUBLANES) * SUBLANES
        self.start = 2 * count - self.rows
        self.shift = count - self.start
        self.places = places
        self.chips = len(places[0][0])
        self.edges = edges
        self.half = half

    def chip(self, side, part, place):
        even, odd = self.places[part][0][place], self.places[part][1][place]
        return even if even == odd else jnp.where(side == 0, even, odd)

    def take(self, pair, low, width, scaled):
        first = self.start if scaled else 0
        found = [ref[:, first : first + self.rows, low : low + width].reshape(-1, width) for ref in pair]
        return jnp.concatenate(found, axis=0)


def in_pairs(flat, parts):
    return [[flat[(lineage * parts + p) * 2 : (lineage * parts + p) * 2 + 2] for p in range(parts)] for lineage in range(2)]


def add_forward(plan, pairs, halves, core, weights, pre):
    gate_ref, up_ref, down_ref = weights
    rows, each = plan.rows, plan.chips // 2
    for lineage in range(2):
        side = core ^ lineage
        for p, (low, high) in enumerate(plan.edges):
            where = pl.ds(pl.multiple_of(side * plan.half + low, LANES), high - low)
            refs = [pairs[lineage][p][h] for h in halves]
            inputs = plan.take(refs, 0, high - low, False)
            scaled = plan.take(refs, 0, high - low, True)
            sums = (
                dot(inputs, gate_ref[where, :], ((1,), (0,))),
                dot(inputs, up_ref[where, :], ((1,), (0,))),
                dot(scaled, down_ref[:, where], ((1,), (1,))),
            )
            for j, h in enumerate(halves):
                for n in range(each):
                    m = plan.chip(side, p, h * each + n)
                    at = (j * each + n) * rows
                    for i, value in enumerate(sums):
                        pre[i, m] += value[at : at + rows]


def finish(plan, pre, delta_ref, hidden_ref):
    rows, chips, units = plan.rows, plan.chips, hidden_ref.shape[2]
    gate_pre, up_pre, back = [pre[i].reshape(chips * rows, units) for i in range(3)]
    total = chips * rows
    if plan.shift:
        back = pltpu.roll(back, total - plan.shift, 0)
    live = lax.broadcasted_iota(jnp.int32, (total, units), 0) % rows < plan.count
    sigmoid = 1.0 / (1.0 + jnp.exp(-gate_pre))
    active = gate_pre * sigmoid
    hidden = jnp.where(live, active * up_pre, 0.0)
    if plan.shift:
        hidden = pltpu.roll(hidden, plan.shift, 0)
    gate_delta = jnp.where(live, back * up_pre * sigmoid * (1.0 + gate_pre * (1.0 - sigmoid)), 0.0)
    up_delta = jnp.where(live, back * active, 0.0)
    delta_ref[:, :, :units] = gate_delta.astype(jnp.bfloat16).reshape(chips, rows, units)
    delta_ref[:, :, units:] = up_delta.astype(jnp.bfloat16).reshape(chips, rows, units)
    hidden_ref[...] = hidden.astype(jnp.bfloat16).reshape(chips, rows, units)


def piece_of(plans):
    return min(PIECE, max(1, 4096 // sum(plan.chips * plan.rows for plan in plans)) * LANES)


def gradients(waves, core):
    plan = waves[0][0]
    piece = piece_of([w[0] for w in waves])
    for lineage in range(2):
        side = core ^ lineage
        for p, (begin, end) in enumerate(plan.edges):
            order = [plan.chip(side, p, place) for place in range(plan.chips)]
            delta = jnp.concatenate([w[2][m] for w in waves for m in order], axis=0)
            hidden = jnp.concatenate([w[3][m] for w in waves for m in order], axis=0)
            for low, high in cut(end - begin, -(-(end - begin) // piece)):
                inputs = jnp.concatenate([w[0].take(w[1][lineage][p], low, high - low, False) for w in waves], axis=0)
                scaled = jnp.concatenate([w[0].take(w[1][lineage][p], low, high - low, True) for w in waves], axis=0)
                tall = dot(inputs, delta, ((0,), (0,)))
                wide = dot(hidden, scaled, ((0,), (0,)))
                yield side, begin + low, high - low, tall, wide


def first_kernel(plans, core_ref, gate_ref, up_ref, down_ref, *rest):
    first, second = plans
    parts = len(first.edges)
    core = core_ref[0]
    weights = (gate_ref, up_ref, down_ref)
    pairs = in_pairs(rest[: 4 * parts], parts)
    rest = rest[4 * parts :]
    early = [[(rest[lineage * parts + p], None) for p in range(parts)] for lineage in range(2)]
    delta_ref, hidden_ref, late, pre = rest[2 * parts :]
    pre[...] = jnp.zeros_like(pre)
    add_forward(first, pairs, (0, 1), core, weights, pre)
    finish(first, pre, delta_ref, hidden_ref)
    late[...] = jnp.zeros_like(late)
    add_forward(second, early, (0,), core, weights, late)


def second_kernel(plans, core_ref, gate_ref, up_ref, down_ref, *rest):
    first, second = plans
    parts = len(first.edges)
    core = core_ref[0]
    weights = (gate_ref, up_ref, down_ref)
    units = gate_ref.shape[1]
    pairs = in_pairs(rest[: 4 * parts], parts)
    first_pairs = in_pairs(rest[4 * parts : 8 * parts], parts)
    first_delta, first_hidden, late = rest[8 * parts : 8 * parts + 3]
    gate_out, up_out, down_out, pre, delta_ref, hidden_ref, tall_held, wide_held, tall_sem, wide_sem = rest[8 * parts + 3 :]
    pre[...] = late[...]
    add_forward(second, pairs, (1,), core, weights, pre)
    waves = [(first, first_pairs, first_delta, first_hidden), (second, pairs, delta_ref, hidden_ref)]
    finish(second, pre, delta_ref, hidden_ref)
    flying = [[], []]
    for turn, (side, low, width, tall, wide) in enumerate(gradients(waves, core)):
        where = pl.ds(pl.multiple_of(side * second.half + low, LANES), width)
        slot = turn % 2
        for copy in flying[slot]:
            copy.wait()
        both = tall.astype(jnp.bfloat16)
        tall_held[slot, 0, :width, :] = both[:, :units]
        tall_held[slot, 1, :width, :] = both[:, units:]
        wide_held[slot, :, :width] = wide.astype(jnp.bfloat16)
        copies = [
            pltpu.make_async_copy(tall_held.at[slot, 0, pl.ds(0, width), :], gate_out.at[where, :], tall_sem.at[slot, 0]),
            pltpu.make_async_copy(tall_held.at[slot, 1, pl.ds(0, width), :], up_out.at[where, :], tall_sem.at[slot, 1]),
            pltpu.make_async_copy(wide_held.at[slot, :, pl.ds(0, width)], down_out.at[:, where], wide_sem.at[slot]),
        ]
        for copy in copies:
            copy.start()
        flying[slot] = copies
    for copies in flying:
        for copy in copies:
            copy.wait()


def on_device(tokens, cotangent, routes, route_gates, gate_weight, up_weight, down_weight):
    units = gate_weight.shape[2]
    slices = HIDDEN_SIZE // units
    window = lax.axis_size("expert") // slices
    width = tokens.shape[1]
    half = width // 2
    me = lax.axis_index("expert").astype(jnp.int32)
    group = (me // slices).reshape(1)
    core = (me % 2).reshape(1)
    smem = pl.BlockSpec(memory_space=pltpu.SMEM)
    vmem = pl.BlockSpec(memory_space=pltpu.VMEM)
    hbm = pl.BlockSpec(memory_space=pl.ANY)

    def near(arrays):
        return [pltpu.with_memory_space_constraint(x, pltpu.VMEM) for x in arrays]

    def far(arrays):
        return [pltpu.with_memory_space_constraint(x, pltpu.HBM) for x in arrays]

    params = pltpu.CompilerParams(vmem_limit_bytes=KERNEL_VMEM)
    folds = 2
    while 2 * CAP * folds % SUBLANES:
        folds *= 2
    span = 2 * CAP * folds
    picked = pl.pallas_call(
        functools.partial(pick_kernel, window, folds),
        out_shape=(jax.ShapeDtypeStruct((span, width // folds), jnp.bfloat16),) * window,
        in_specs=[smem] + [hbm] * 4,
        out_specs=(vmem,) * window,
        scratch_shapes=[
            pltpu.VMEM(routes.shape[::-1], routes.dtype),
            pltpu.VMEM(route_gates.shape[::-1], route_gates.dtype),
            pltpu.VMEM(tokens.shape, tokens.dtype),
            pltpu.VMEM(cotangent.shape, cotangent.dtype),
            pltpu.SemaphoreType.DMA((2,)),
            pltpu.SemaphoreType.DMA((folds, 2)),
        ],
        compiler_params=pltpu.CompilerParams(vmem_limit_bytes=PICK_VMEM),
    )(group, *far((routes.T, route_gates.T, tokens, cotangent)))
    weights = far((gate_weight[0], up_weight[0], down_weight[0]))
    weights = pl.pallas_call(
        functools.partial(load_kernel, len(weights)),
        out_shape=tuple(jax.ShapeDtypeStruct(w.shape, w.dtype) for w in weights),
        in_specs=[hbm] * (len(weights) + 1),
        out_specs=(vmem,) * len(weights),
        scratch_shapes=[pltpu.SemaphoreType.DMA((len(weights),))],
        cost_estimate=pl.CostEstimate(flops=1 << 32, bytes_accessed=12 * width * units, transcendentals=0),
        compiler_params=params,
    )(*weights, picked[0])
    partner = (1, 0)
    landed = [picked[0]]
    for k in range(1, window):
        landed.append(hop(picked[k], (k * slices, 0)))
    pairs = []
    for block in landed:
        pairs.append((block, hop(block, partner)))

    dims = [(0, m) for m in bits_of(lax.axis_size("dp"))] + [(m, 0) for m in bits_of(slices)[1:]]
    tiles = half // LANES
    major = -(-2 * tiles // len(dims)) * LANES
    edges = [(0, major), (major, half)]
    orders = [(turned(dims, 0), turned(dims, 2)), (turned(dims, 1), turned(dims, 1))]
    places = [tuple(masks_of(o, dims) for o in order) for order in orders]
    main = CAP // SUBLANES * SUBLANES
    early = [(0, 0, main, 0)]
    late = [(k, 0, CAP, (k - 1) * 2 * CAP) for k in range(1, window)]
    if main < CAP:
        late.append((0, main, CAP, (window - 1) * 2 * CAP))
    plans, operands, gathered = [], [], []
    for taken in (early, late):
        count = sum(2 * (high - low) for _, low, high, _ in taken)
        count += -count % (SUBLANES // 2)
        sources = [x for k, _, _, _ in taken for x in pairs[k]]
        entries = [(flip, low, high, start) for _, low, high, start in taken for flip in range(2)]
        blocks = pl.pallas_call(
            functools.partial(join_kernel, folds, edges, entries),
            out_shape=tuple(jax.ShapeDtypeStruct((2 * count, high - low), jnp.bfloat16) for low, high in edges),
            in_specs=[smem] + [vmem] * len(sources),
            out_specs=(vmem,) * len(edges),
            compiler_params=params,
        )(core, *near(sources))
        halves = gather_cube(blocks, orders)
        gathered.append(halves)
        stacks = [s for pair in halves for s in pair]
        crossed = []
        for stack in stacks:
            crossed.append(hop(stack, partner))
        operands.append(stacks + crossed)
        plans.append(Plan(count, places, edges, half))

    chips = plans[0].chips

    def of_rows(plan, make):
        return [make((chips, plan.rows, 2 * units), jnp.bfloat16), make((chips, plan.rows, units), jnp.bfloat16)]

    def sums(plan, make):
        return make((3, chips, plan.rows, units), jnp.float32)

    flops = [6 * chips * plan.rows * width * units for plan in plans]
    held, _ = lax.optimization_barrier((operands[0] + operands[1][::2], gathered[1][0][0]))
    shapes = of_rows(plans[0], jax.ShapeDtypeStruct) + [sums(plans[1], jax.ShapeDtypeStruct)]
    first = pl.pallas_call(
        functools.partial(first_kernel, plans),
        out_shape=tuple(shapes),
        in_specs=[smem] + [vmem] * (3 + len(held)),
        out_specs=(vmem,) * len(shapes),
        scratch_shapes=[sums(plans[0], pltpu.VMEM)],
        cost_estimate=pl.CostEstimate(flops=2 * flops[0], bytes_accessed=6 * width * units, transcendentals=0),
        compiler_params=params,
    )(core, *near(weights), *near(held))
    extra = near(held[: len(operands[0])]) + near(first)
    grads = pl.pallas_call(
        functools.partial(second_kernel, plans),
        out_shape=(
            jax.ShapeDtypeStruct((width, units), jnp.bfloat16),
            jax.ShapeDtypeStruct((width, units), jnp.bfloat16),
            jax.ShapeDtypeStruct((units, width), jnp.bfloat16),
        ),
        in_specs=[smem] + [vmem] * (3 + len(operands[1]) + len(extra)),
        out_specs=(hbm, hbm, hbm),
        scratch_shapes=[sums(plans[1], pltpu.VMEM)]
        + of_rows(plans[1], pltpu.VMEM)
        + [
            pltpu.VMEM((2, 2, piece_of(plans), units), jnp.bfloat16),
            pltpu.VMEM((2, units, piece_of(plans)), jnp.bfloat16),
            pltpu.SemaphoreType.DMA((2, 2)),
            pltpu.SemaphoreType.DMA((2,)),
        ],
        cost_estimate=pl.CostEstimate(flops=2 * sum(flops), bytes_accessed=12 * width * units, transcendentals=0),
        compiler_params=params,
    )(core, *near(weights), *near(operands[1]), *extra)
    return tuple(g[None] for g in grads)


def solution(mesh):
    split = P(("expert", "dp"), None)
    held = P("expert", None, None)

    return jax.shard_map(
        on_device,
        mesh=mesh,
        in_specs=(split, split, split, split, held, held, held),
        out_specs=(held, held, held),
        check_vma=False,
    )
```
